512 devices in a mesh: seq: 128 (over z, y, core), grp: 4 (over x).
Axes of the slice: x: 4, y: 4, z: 16, core: 2. Of those that a mesh axis runs over, the one named last changes fastest.
Arguments:
- query_nope: bfloat16 [4, 2, 128, 128], P(None, None, 'seq'), may hold values from -12.859821 to 12.859821
- query_rope: bfloat16 [4, 2, 128, 64], P(None, None, 'seq'), may hold values from -150 to 150
- latent_cache: bfloat16 [4, 131072, 576], P(None, ('seq', 'grp')), may hold values from -5 to 5
- lengths: int32 [4], replicated, may hold values from 65536 to 131072
- key_weight: bfloat16 [128, 128, 512], P('seq'), may hold values from -0.5 to 0.5
- value_weight: bfloat16 [128, 512, 128], P('seq'), may hold values from -0.25 to 0.25
- output_weight: bfloat16 [16384, 7168], P('seq', 'grp'), may hold values from -0.1875 to 0.1875
Outputs:
- mixed: bfloat16 [4, 2, 7168], P(None, None, ('grp', 'seq'))
The draws below stay inside these ranges and needn't reach their ends.
All inputs are finite; a program needn't handle non-finite values.
Results may differ from the reference program's by a relative error of at most 0.0095.
Values may be sent and summed in bfloat16 or wider, within the bound.
A program may use at most 64 MiB of HBM per device.

```python
import math
import jax
import jax.numpy as jnp
from jax import lax

H = 128
DL = 512
DR = 64
DN = 128
DV = 128
DM = 7168
B = 4
QT = 2
CTX_DEV = 256
SEQ = 131072
N_SEQ = 128
N_GRP = 4


echo_shrink = 0.008


def anchor_plan(key):
    subkeys = jax.random.split(jax.random.fold_in(key, 613), 8)
    sign_flip = jnp.where(jax.random.bernoulli(subkeys[0], 0.5, (B, DR)), 1.0, -1.0)
    anchor = 5.0 * sign_flip * jax.random.uniform(subkeys[1], (B, DR), jnp.float32, 0.8, 1.0)
    anchor_at = jax.random.randint(subkeys[2], (B,), 0, SEQ // 4 - 1)
    class_pick = jax.random.uniform(subkeys[3], (B, QT, H, 1), jnp.float32)
    strong_heads = class_pick < -1.0
    drawn_heads = jnp.logical_and(class_pick >= 0.125, class_pick < 0.375)
    drawn_target = jax.random.uniform(subkeys[4], (B, QT, H, 1), jnp.float32, 11.0, 15.0)
    strong_target = jax.random.uniform(subkeys[5], (B, QT, H, 1), jnp.float32, 150.0, 330.0)
    blend = jax.random.uniform(subkeys[6], (B, QT, H, 1), jnp.float32, 0.0, 1.5)
    crosswise = jax.random.normal(subkeys[7], (B, QT, H, DR), jnp.float32)
    return (anchor, anchor_at, strong_heads, drawn_heads, drawn_target, strong_target, blend, crosswise)


def draw_latent_cache(key, part):
    anchor, anchor_at, strong_heads, drawn_heads, drawn_target, strong_target, blend, crosswise = anchor_plan(key)
    subkeys = jax.random.split(jax.random.fold_in(key, 271), 3)
    latent = jnp.clip(jax.random.normal(subkeys[1], (B, SEQ, DL), jnp.float32), -5.0, 5.0)
    rotary = jnp.clip(jax.random.normal(subkeys[2], (B, SEQ, DR), jnp.float32), -5.0, 5.0)
    positions = jnp.arange(SEQ, dtype=jnp.int32)[None, :, None]
    anchor_rows = anchor[:, None, :]
    rotary = jnp.where(positions == anchor_at[:, None, None], anchor_rows, rotary)
    rotary = jnp.where(positions == (anchor_at + SEQ // 4)[:, None, None], anchor_rows * (1.0 - echo_shrink), rotary)
    return jnp.concatenate([latent, rotary], axis=-1).astype(jnp.bfloat16)


def draw_query_nope(key, part):
    anchor, anchor_at, strong_heads, drawn_heads, drawn_target, strong_target, blend, crosswise = anchor_plan(key)
    spread = 3.5 * math.sqrt(DN + DR) / math.sqrt(DL)
    nope_key = jax.random.fold_in(key, 419)
    drawn_draw = jnp.clip(jax.random.normal(nope_key, (B, QT, H, DN), jnp.float32), -6.0, 6.0)
    factor = jnp.where(strong_heads, 0.1, jnp.where(drawn_heads, 0.4, 1.0))
    return (spread * factor * drawn_draw).astype(jnp.bfloat16)


def draw_query_rope(key, part):
    anchor, anchor_at, strong_heads, drawn_heads, drawn_target, strong_target, blend, crosswise = anchor_plan(key)
    rope_key = jax.random.fold_in(key, 523)
    drawn_draw = jnp.clip(2.0 * jax.random.normal(rope_key, (B, QT, H, DR), jnp.float32), -12.0, 12.0)
    anchors = anchor[:, None, None, :]
    squared = jnp.sum(anchors * anchors, axis=-1, keepdims=True)
    parallel = jnp.sum(crosswise * anchors, axis=-1, keepdims=True) / squared
    across = crosswise - parallel * anchors
    across = across / jnp.sqrt(jnp.sum(across * across, axis=-1, keepdims=True) + 1e-06)
    direction = anchors + blend * jnp.sqrt(squared) * across
    root_width = math.sqrt(DN + DR)
    strong_query = strong_target * root_width / squared * direction
    drawn_query = drawn_target * root_width / squared * anchors
    queries = jnp.where(strong_heads, strong_query, jnp.where(drawn_heads, drawn_query, drawn_draw))
    return jnp.clip(queries, -150.0, 150.0).astype(jnp.bfloat16)


def plant(result, stream_key, smallest, high):
    place = [jax.random.randint(jax.random.fold_in(stream_key, axis), (), 0, length) for axis, length in enumerate(result.shape)]
    widest = result.shape.index(max(result.shape))
    next_to = place[:widest] + [(place[widest] + 1) % result.shape[widest]] + place[widest + 1:]
    return result.at[tuple(place)].set(smallest).at[tuple(next_to)].set(high)


def spiked(array, own_key, source, target, blocks, factor):
    owner, partner = [(jnp.arange(array.shape[axis_at]) // (array.shape[axis_at] // blocks)).reshape([-1 if axis == axis_at else 1 for axis in range(array.ndim)]) for axis_at in (source, target)]
    chosen = jax.random.permutation(own_key, blocks)[partner]
    strong = (owner == chosen) | (owner == (partner + blocks // 2) % blocks)
    return jnp.where(strong, factor * array, array)


def levels(own_key, extent, pieces, low, largest):
    def one(dim, shards_of):
        steps = jax.random.uniform(jax.random.fold_in(jax.random.fold_in(own_key, 6), dim), (shards_of,), jnp.float32, low / len(pieces), largest / len(pieces))
        return jnp.repeat(jnp.exp(steps), extent[dim] // shards_of).reshape((-1,) + (1,) * (len(extent) - dim - 1))

    level = one(*pieces[0])
    for cut in pieces[1:]:
        level = level * one(*cut)
    return level


def scatter_about(own_key, extent, deviation, reach, cuts=(), held_as=jnp.bfloat16):
    values = deviation * jax.random.normal(own_key, extent, jnp.float32)
    if cuts:
        values = values * levels(own_key, extent, cuts, -0.22, 0.18)
    return jnp.clip(values, -reach, reach).astype(held_as)


def gaussian_with(own_key, extent, scale, reach, cuts, heavy, held_as=jnp.bfloat16):
    array = scale * jax.random.normal(own_key, extent, jnp.float32)
    if cuts:
        array = array * levels(own_key, extent, cuts, -0.22, 0.18)
    return jnp.clip(spiked(array, jax.random.fold_in(own_key, 3), *heavy), -reach, reach).astype(held_as)


def setup_inputs(seed: int = 0) -> dict:
    seeds = jax.random.split(jax.random.key(seed), 8)
    return {
        "query_nope": draw_query_nope(jax.random.fold_in(seeds[7], 71), 0),
        "query_rope": draw_query_rope(jax.random.fold_in(seeds[7], 71), 0),
        "latent_cache": draw_latent_cache(jax.random.fold_in(seeds[7], 71), 0),
        "lengths": plant(jax.random.randint(seeds[3], (B,), SEQ // 2, SEQ + 1), jax.random.fold_in(seeds[3], 1), SEQ // 2, SEQ).astype(jnp.int32),
        "key_weight": scatter_about(seeds[4], (H, DN, DL), DN ** -0.5, 0.5, ((0, 128),)),
        "value_weight": scatter_about(seeds[5], (H, DL, DV), DL ** -0.5, 0.25, ((0, 128),)),
        "output_weight": gaussian_with(seeds[6], (H * DV, DM), (H * DV) ** -0.5, 0.1875, ((0, 128), (1, 4)), (0, 1, 128, 5.5)),
    }


NEGATIVE = -1e30


def shard_partial(queries, cache_block, limits, offset):
    raw_score = jnp.einsum("bqhd,bpd->bqhp", queries.astype(jnp.float32), cache_block.astype(jnp.float32)) * ((DN + DR) ** -0.5)
    places = offset + jnp.arange(CTX_DEV, dtype=jnp.int32)
    visible = places[None, None, :] < limits[:, :, None]
    scores = jnp.where(visible[:, :, None, :], raw_score, NEGATIVE)
    maxima = jnp.max(scores, axis=-1)
    powers = jnp.exp(scores - maxima[..., None])
    totals = jnp.sum(powers, axis=-1)
    weights = lax.optimization_barrier(powers.astype(jnp.bfloat16))
    summed = jnp.einsum("bqhp,bpd->bqhd", weights.astype(jnp.float32), cache_block[:, :, :DL].astype(jnp.float32))
    partials = (summed / totals[..., None]).astype(jnp.bfloat16)
    return maxima, totals, partials


def reference(query_nope, query_rope, latent_cache, lengths, key_weight, value_weight, output_weight):
    absorbed = jnp.einsum("bqhn,hnd->bqhd", query_nope.astype(jnp.float32), key_weight.astype(jnp.float32))
    absorbed = absorbed.astype(jnp.bfloat16)
    queries = jnp.concatenate([absorbed, query_rope], axis=-1)
    limits = lengths[:, None] - QT + 1 + jnp.arange(QT, dtype=jnp.int32)[None, :]

    def visit_shard(carried, shard_index):
        highest, summed, numerator = carried
        offset = (shard_index * CTX_DEV).astype(jnp.int32)
        cache_block = lax.dynamic_slice_in_dim(latent_cache, offset, CTX_DEV, 1)
        maxima, totals, partials = shard_partial(queries, cache_block, limits, offset)
        partials = lax.optimization_barrier(partials)
        raised = jnp.maximum(highest, maxima)
        rescale = jnp.exp(highest - raised)
        shares = totals * jnp.exp(maxima - raised)
        numerator = numerator * rescale[..., None] + shares[..., None] * partials.astype(jnp.float32)
        return (raised, summed * rescale + shares, numerator), None

    start_state = (jnp.full((B, QT, H), NEGATIVE, jnp.float32), jnp.zeros((B, QT, H), jnp.float32), jnp.zeros((B, QT, H, DL), jnp.float32))
    final_state, unused = lax.scan(visit_shard, start_state, jnp.arange(N_SEQ * N_GRP, dtype=jnp.int32))
    latent_out = lax.optimization_barrier((final_state[2] / final_state[1][..., None]).astype(jnp.bfloat16))
    values = jnp.einsum("bqhd,hde->bqhe", latent_out.astype(jnp.float32), value_weight.astype(jnp.float32)).astype(jnp.bfloat16)
    projected = jnp.dot(values.reshape(B * QT, H * DV), output_weight, preferred_element_type=jnp.float32)
    return projected.reshape(B, QT, DM).astype(jnp.bfloat16)
```

```python
import functools

import jax
import jax.numpy as jnp
from jax import lax
from jax.experimental import pallas as pl
from jax.experimental.pallas import tpu as pltpu
from jax.sharding import Mesh
from jax.sharding import PartitionSpec as P

SEQ = ("z", "y", "c")
SEQ_GRP = ("z", "y", "c", "x")
GRP_SEQ = ("x", "z", "y", "c")
MESH = pl.DeviceIdType.MESH
NEGATIVE = -1e30
F32, BF16 = jnp.float32, jnp.bfloat16


def ring_offsets(n):
    order = [0]
    for d in range(1, n // 2):
        order += [d, -d]
    return order + [n // 2] if n > 1 else order


def by_distance(n):
    return sorted(range(n), key=lambda d: (-min(d, n - d), d))


def kernel(
    dims, factor,
    qn_hbm, qr_hbm, kv_hbm, len_hbm, kw_hbm, vw_hbm, ow_hbm,
    out_ref,
    qn, qr, lens, kw, vw, ow, kv,
    qz, qf, qall,
    osend, orecv, ssend, srecv,
    zf, zsend, zrecv,
    vx, vf,
    czsend, czrecv, cysend, cyrecv,
    local_sem, kv_sem, z_sem, xy_sem, o_sem, s_sem, b_sem, v_sem, cz_sem, cy_sem,
):
    nz, ny, nc, nx = dims
    z, y, c, x = (lax.axis_index(a) for a in SEQ_GRP)
    offs = ring_offsets(nz)
    half = nz // 2
    dl = kw.shape[1]
    ctx = kv.shape[2]
    rows = 2 * nz * ny
    wide = 2 * half
    plane = [(dx, dy) for dx in by_distance(nx) for dy in by_distance(ny) if (dx, dy) != (0, 0)]

    def near(v, d, n):
        return lax.rem(v + (d % n), n)

    barrier = pltpu.get_barrier_semaphore()
    peers = 0
    for k in range(nz - 1, 0, -1):
        pl.semaphore_signal(barrier, inc=1, device_id={"z": near(z, offs[k], nz)}, device_id_type=MESH)
        peers += 1
    for dx, dy in plane:
        pl.semaphore_signal(
            barrier, inc=1, device_id={"x": near(x, dx, nx), "y": near(y, dy, ny)}, device_id_type=MESH
        )
        peers += 1
    for dy in range(ny):
        pl.semaphore_signal(
            barrier, inc=1, device_id={"y": near(y, dy, ny), "c": 1 - c}, device_id_type=MESH
        )
        peers += 1

    loads = [
        pltpu.make_async_copy(src, dst, local_sem.at[i])
        for i, (src, dst) in enumerate(
            [
                (qn_hbm, qn), (qr_hbm, qr), (kw_hbm.at[0], kw), (kv_hbm, kv.at[c]),
                (len_hbm, lens), (vw_hbm.at[0], vw), (ow_hbm, ow),
            ]
        )
    ]
    for load in loads:
        load.start()

    for i in (0, 1, 2):
        loads[i].wait()
    absorbed = jnp.dot(qn[x], kw[...], preferred_element_type=F32)
    qz[0, :, :dl] = absorbed.astype(BF16)
    qz[0, :, dl:] = qr[x]

    pl.semaphore_wait(barrier, peers)

    started = []

    def send(src, dst, sems, at, device):
        copy = pltpu.make_async_remote_copy(
            src_ref=src, dst_ref=dst, send_sem=sems.at[(0, *at)], recv_sem=sems.at[(1, *at)],
            device_id=device, device_id_type=MESH,
        )
        copy.start()
        started.append(copy)
        return copy

    zcopies = {}
    for k in range(nz - 1, 0, -1):
        zcopies[k] = send(qz.at[0], qz.at[k], z_sem, (k,), {"z": near(z, -offs[k], nz)})
    kvcopy = send(kv_hbm, kv.at[c], kv_sem, (0,), {"c": 1 - c})

    xycopies = []
    for g in range(2):
        for i in range(half):
            k = g * half + i
            if k:
                zcopies[k].wait_recv()
            qf[2 * i : 2 * i + 2, :] = qz[k].astype(F32)
        qall[x, g, y] = qf[...].astype(BF16)
        for dx, dy in plane:
            xycopies.append(
                send(
                    qall.at[x, g, y], qall.at[x, g, y], xy_sem, (g, dx * ny + dy),
                    {"x": near(x, dx, nx), "y": near(y, dy, ny)},
                )
            )

    for i in (3, 4):
        loads[i].wait()
    kvcopy.wait_recv()
    for copy in xycopies:
        copy.wait_recv()

    row = lax.broadcasted_iota(jnp.int32, (rows, ctx), 0)
    place = lax.broadcasted_iota(jnp.int32, (rows, ctx), 1)
    drafts = lax.rem(row, 2)
    eye = lax.broadcasted_iota(jnp.int32, (rows, rows), 0) == lax.broadcasted_iota(
        jnp.int32, (rows, rows), 1
    )
    ocopies, scopies = {}, {}
    for dx in by_distance(nx):
        b = near(x, dx, nx)
        q = qall[b].reshape(rows, qall.shape[-1])
        limit = lens[b] - 1 + drafts
        scores, seen = [], []
        for e in range(nc):
            start = (((z * ny + y) * nc + e) * nx + x) * ctx
            raw = lax.dot_general(
                q, kv[e, b], (((1,), (1,)), ((), ())), preferred_element_type=F32
            ) * factor
            seen.append(place + start < limit)
            scores.append(jnp.where(seen[e], raw, NEGATIVE))
        top = functools.reduce(jnp.maximum, [jnp.max(s, axis=1, keepdims=True) for s in scores])
        expo = [jnp.where(m, jnp.exp(s - top), 0.0) for m, s in zip(seen, scores)]
        total = sum(jnp.sum(e, axis=1, keepdims=True) for e in expo)
        numer = sum(
            jnp.dot(expo[e].astype(BF16), kv[e, b, :, :dl], preferred_element_type=F32)
            for e in range(nc)
        )
        blocks = numer.astype(BF16).reshape(2, ny, wide, dl)
        for g in range(2):
            osend[b, :, g] = blocks[g]
        ssend[b, 0:1, :] = jnp.sum(jnp.where(eye, top, 0.0), axis=0, keepdims=True)
        ssend[b, 1:2, :] = jnp.sum(jnp.where(eye, total, 0.0), axis=0, keepdims=True)
        for dy in by_distance(ny):
            if (dx, dy) == (0, 0):
                continue
            device = {"x": b, "y": near(y, dy, ny)}
            j = dx * ny + dy
            scopies[j] = send(ssend.at[b], srecv.at[j], s_sem, (j,), device)
            ocopies[j] = send(osend.at[b, near(y, dy, ny)], orecv.at[j], o_sem, (j,), device)

    order = [0] + [dx * ny + dy for dx, dy in reversed(plane)]
    for j in order[1:]:
        scopies[j].wait_recv()
    stats = {j: (ssend[x] if j == 0 else srecv[j]) for j in order}
    peak = functools.reduce(jnp.maximum, [stats[j][0:1] for j in order])
    peak_hi = peak.astype(BF16).astype(F32)
    peak_lo = (peak - peak_hi).astype(BF16).astype(F32)
    level = peak_hi + peak_lo
    scale = {j: jnp.exp(jnp.minimum(stats[j][0:1] - level, 16.0)) for j in order}
    denom = sum(scale[j] * stats[j][1:2] for j in order)
    denom_hi = denom.astype(BF16).astype(F32)
    denom_lo = (denom - denom_hi).astype(BF16).astype(F32)

    own = lax.broadcasted_iota(jnp.int32, (2 * wide, rows), 0)
    own = lax.div(own, wide) * (ny * wide) + y * wide + lax.rem(own, wide)
    pick = own == lax.broadcasted_iota(jnp.int32, (2 * wide, rows), 1)

    def column(values):
        return jnp.sum(jnp.where(pick, values, 0.0), axis=1, keepdims=True)

    merged = None
    for j in order:
        if j:
            ocopies[j].wait_recv()
        block = osend[x, y] if j == 0 else orecv[j]
        term = column(scale[j]) * block.reshape(2 * wide, dl).astype(F32)
        merged = term if merged is None else merged + term
    zf[:, :dl] = merged
    lane = lax.broadcasted_iota(jnp.int32, (2 * wide, 128), 1)
    zf[:, dl:] = jnp.where(
        lane < 64,
        jnp.where(lane < 32, column(peak_hi), column(peak_lo)),
        jnp.where(lane < 96, column(denom_hi), column(denom_lo)),
    )
    for k in range(nz):
        zsend[k] = zf[2 * k : 2 * k + 2, :].astype(BF16)

    bcopies = {}
    for k in range(nz - 1, 0, -1):
        bcopies[k] = send(zsend.at[k], zrecv.at[k], b_sem, (k,), {"z": near(z, offs[k], nz)})
    for i in (5, 6):
        loads[i].wait()
    parts = []
    for k in range(nz):
        if k:
            bcopies[k].wait_recv()
        parts.append((zrecv[k] if k else zsend[0]).astype(F32))
    tops = [p[:, dl : dl + 1] + p[:, dl + 32 : dl + 33] for p in parts]
    sums = [p[:, dl + 64 : dl + 65] + p[:, dl + 96 : dl + 97] for p in parts]
    highest = functools.reduce(jnp.maximum, tops)
    shares = [jnp.exp(t - highest) for t in tops]
    bottom = sum(s * t for s, t in zip(shares, sums))
    latent = sum(s * p[:, :dl] for s, p in zip(shares, parts)) / bottom
    values = jnp.dot(latent.astype(BF16), vw[...], preferred_element_type=F32)
    vx[x] = values.astype(BF16)

    vcopies = [
        send(vx.at[x], vx.at[x], v_sem, (dx,), {"x": near(x, dx, nx)})
        for dx in by_distance(nx)
        if dx
    ]
    for copy in vcopies:
        copy.wait_recv()
    for b in range(nx):
        vf[2 * b : 2 * b + 2, :] = vx[b].astype(F32)
    terms = jnp.dot(vf[...].astype(BF16), ow[...], preferred_element_type=F32)

    cols = czsend.shape[2]
    for j in range(nz):
        czsend[j] = terms[:, j * cols : (j + 1) * cols].astype(BF16)
    czcopies = {}
    for k in range(nz - 1, 0, -1):
        dest = near(z, offs[k], nz)
        czcopies[k] = send(czsend.at[dest], czrecv.at[k], cz_sem, (k,), {"z": dest})
    summed = czsend[z].astype(F32)
    for k in range(1, nz):
        czcopies[k].wait_recv()
        summed = summed + czrecv[k].astype(F32)
    cysend[...] = summed
    cycopies = {}
    for dy in by_distance(ny):
        for dc in range(nc - 1, -1, -1):
            if (dy, dc) == (0, 0):
                continue
            j = dy * nc + dc
            cycopies[j] = send(
                cysend, cyrecv.at[j], cy_sem, (j,),
                {"y": near(y, dy, ny), "c": near(c, dc, nc)},
            )
    for j in range(1, ny * nc):
        cycopies[j].wait_recv()
        summed = summed + cyrecv[j]
    width = cols // (ny * nc)
    mine = y * nc + c
    result = summed[:, :width]
    for j in range(1, ny * nc):
        result = jnp.where(mine == j, summed[:, j * width : (j + 1) * width], result)
    out_ref[...] = result.astype(BF16)

    for copy in started:
        copy.wait_send()


def shards(dims, query_nope, query_rope, latent_cache, lengths, key_weight, value_weight, output_weight):
    nz, ny, nc, nx = dims
    dn, dr = query_nope.shape[3], query_rope.shape[3]
    dl, dv = key_weight.shape[2], value_weight.shape[2]
    nb, ctx, dk = latent_cache.shape
    dm = output_weight.shape[1]
    assert nb == nx and query_nope.shape[1] == 2 and query_nope.shape[2] == 1
    half = nz // 2
    wide = 2 * half
    rows = 2 * nz * ny
    cols = dm // nz
    factor = float(dn + dr) ** (-0.5)
    dma = pltpu.SemaphoreType.DMA
    hbm = pl.BlockSpec(memory_space=pl.ANY)
    result = pl.pallas_call(
        functools.partial(kernel, dims, factor),
        out_shape=jax.ShapeDtypeStruct((2 * nb, cols // (ny * nc)), BF16),
        in_specs=[hbm] * 7,
        out_specs=pl.BlockSpec(memory_space=pltpu.VMEM),
        scratch_shapes=[
            pltpu.VMEM((nb, 2, dn), BF16),
            pltpu.VMEM((nb, 2, dr), BF16),
            pltpu.SMEM((nb,), jnp.int32),
            pltpu.VMEM((dn, dl), BF16),
            pltpu.VMEM((dl, dv), BF16),
            pltpu.VMEM((dv, dm), BF16),
            pltpu.VMEM((nc, nb, ctx, dk), BF16),
            pltpu.VMEM((nz, 2, dk), BF16),
            pltpu.VMEM((wide, dk), F32),
            pltpu.VMEM((nb, 2, ny, wide, dk), BF16),
            pltpu.VMEM((nb, ny, 2, wide, dl), BF16),
            pltpu.VMEM((nx * ny, 2, wide, dl), BF16),
            pltpu.VMEM((nb, 2, rows), F32),
            pltpu.VMEM((nx * ny, 2, rows), F32),
            pltpu.VMEM((2 * wide, dl + 128), F32),
            pltpu.VMEM((nz, 2, dl + 128), BF16),
            pltpu.VMEM((nz, 2, dl + 128), BF16),
            pltpu.VMEM((nb, 2, dv), BF16),
            pltpu.VMEM((2 * nb, dv), F32),
            pltpu.VMEM((nz, 2 * nb, cols), BF16),
            pltpu.VMEM((nz, 2 * nb, cols), BF16),
            pltpu.VMEM((2 * nb, cols), F32),
            pltpu.VMEM((ny * nc, 2 * nb, cols), F32),
            dma((7,)),
            dma((2, 1)),
            dma((2, nz)),
            dma((2, 2, nx * ny)),
            dma((2, nx * ny)),
            dma((2, nx * ny)),
            dma((2, nz)),
            dma((2, nx)),
            dma((2, nz)),
            dma((2, ny * nc)),
        ],
        compiler_params=pltpu.CompilerParams(collective_id=0, has_side_effects=True),
    )(
        query_nope.reshape(nb, 2, dn),
        query_rope.reshape(nb, 2, dr),
        latent_cache,
        lengths,
        key_weight,
        value_weight,
        output_weight,
    )
    return result.reshape(nb, 2, -1)


def solution_dims(mesh, dims):
    split = Mesh(mesh.devices.reshape(dims), SEQ_GRP)
    in_specs = (
        P(None, None, SEQ, None),
        P(None, None, SEQ, None),
        P(None, SEQ_GRP, None),
        P(),
        P(SEQ, None, None),
        P(SEQ, None, None),
        P(SEQ, "x"),
    )
    return jax.shard_map(
        functools.partial(shards, dims),
        mesh=split,
        in_specs=in_specs,
        out_specs=P(None, None, GRP_SEQ),
        check_vma=False,
    )


def solution(mesh):
    ny, nc = 4, 2
    nz = mesh.shape["seq"] // (ny * nc)
    return solution_dims(mesh, (nz, ny, nc, mesh.shape["grp"]))
```
